32 devices in a mesh: fsdp: 8 (over z, y), tp: 4 (over x, core).
Axes of the slice: x: 2, y: 2, z: 4, core: 2. Of those that a mesh axis runs over, the one named last changes fastest.
Arguments:
- gate_weight: bfloat16 [4096, 11008], P('fsdp', 'tp'), may hold values from -6 to 6
- up_weight: bfloat16 [4096, 11008], P('fsdp', 'tp'), may hold values from -6 to 6
- down_weight: bfloat16 [11008, 4096], P('tp', 'fsdp'), may hold values from -6 to 6
- source_map: int32 [11008], P(('fsdp', 'tp')), may hold values from 0 to 11007
Outputs:
- added_gate: bfloat16 [4096, 11008], P('fsdp', 'tp')
- added_up: bfloat16 [4096, 11008], P('fsdp', 'tp')
- kept_down: bfloat16 [11008, 4096], P('tp', 'fsdp')
- added_down: bfloat16 [11008, 4096], P('tp', 'fsdp')
The draws below stay inside these ranges and needn't reach their ends.
Inputs may be any that keep to these rules, and one draw needn't show every extreme that they name: `source_map`: each entry names an initial hidden unit; some units are named many times, many not at all.
All inputs are finite; a program needn't handle non-finite values.
Results may differ from the reference program's by a relative error of at most 0.001.
Values may be sent and summed in bfloat16 or wider, within the bound.
No kernel may reach another device: no remote copies, remote signals or barrier semaphores. Data moves between devices by JAX's collectives and lax.ppermute only.
A program may use at most 128 MiB of HBM per device.

```python
import math
import jax
import jax.numpy as jnp
import numpy as np

D = 4096
FF = 11008
EXTRA = 11008


def plant(drawn, stream_key, smallest, top_value):
    dims = drawn.shape
    spot = [jax.random.randint(jax.random.fold_in(stream_key, axis), (), 0, dims[axis]) for axis in range(len(dims))]
    drawn = drawn.at[tuple(spot)].set(smallest)
    longest = dims.index(max(dims))
    spot[longest] = (spot[longest] + 1) % dims[longest]
    return drawn.at[tuple(spot)].set(top_value)


def steps_of(stream_key, shape, split, low, top_value):
    def one(position, parts):
        heights = jax.random.uniform(jax.random.fold_in(jax.random.fold_in(stream_key, 6), position), (parts,), jnp.float32, low / len(split), top_value / len(split))
        return jnp.repeat(jnp.exp(heights), shape[position] // parts).reshape((-1,) + (1,) * (len(shape) - position - 1))

    factor_of = one(*split[0])
    for cut in split[1:]:
        factor_of = factor_of * one(*cut)
    return factor_of


def cumulative_ranks(number_of, slope):
    portions = [(1 << 20) // math.isqrt(rank ** slope) + 1 for rank in range(1, number_of + 1)]
    spread = 1 + sum(portions) // (1 << 30)
    return np.cumsum(np.array([max(1, weight // spread) for weight in portions]))


def ranked(own_key, shape, amount, slope):
    grid = cumulative_ranks(amount, slope)
    lot = jax.random.randint(jax.random.fold_in(own_key, 1), shape, 0, int(grid[amount - 1]))
    grade = jnp.searchsorted(jnp.asarray(grid, jnp.int32), lot, side="right")
    return jax.random.permutation(jax.random.fold_in(own_key, 2), amount)[grade].astype(jnp.int32)


def noise(key, shape, deviation, bound, split=(), kind=jnp.bfloat16):
    level = steps_of(key, shape, split, -0.22, 0.18) if split else 1.0
    array = jax.random.normal(key, shape, jnp.float32) * deviation * level
    return jnp.minimum(jnp.maximum(array, -bound), bound).astype(kind)


def setup_inputs(seed: int = 0) -> dict:
    keys = jax.random.split(jax.random.key(seed), 5)
    return {
        "gate_weight": noise(keys[0], (D, FF), 1.0, 6.0, ((0, 8), (1, 4))),
        "up_weight": noise(keys[1], (D, FF), 1.0, 6.0, ((0, 8), (1, 4))),
        "down_weight": noise(keys[2], (FF, D), 1.0, 6.0, ((0, 4), (1, 8))),
        "source_map": plant(ranked(keys[3], (EXTRA,), FF, 1), jax.random.fold_in(keys[3], 3), 0, FF - 1).astype(jnp.int32),
    }


def reference(gate_weight, up_weight, down_weight, source_map):
    counts = jnp.ones((FF,), jnp.float32).at[source_map].add(jnp.ones(source_map.shape, jnp.float32))
    added_gate = jnp.take(gate_weight, source_map, axis=1)
    added_up = jnp.take(up_weight, source_map, axis=1)
    kept_down = (down_weight.astype(jnp.float32) / counts[:, None]).astype(jnp.bfloat16)
    picked = jnp.take(down_weight, source_map, axis=0).astype(jnp.float32)
    added_down = (picked / jnp.take(counts, source_map)[:, None]).astype(jnp.bfloat16)
    return (added_gate, added_up, kept_down, added_down)
```

```python
import functools

import jax
import jax.numpy as jnp
from jax import lax
from jax.experimental import pallas as pl
from jax.experimental.pallas import tpu as pltpu
from jax.sharding import PartitionSpec as P


LANES = 128
F32, BF16, I32 = jnp.float32, jnp.bfloat16, jnp.int32


def ceil_to(value, unit):
    return -(-value // unit) * unit


def iota(shape, axis):
    return lax.broadcasted_iota(I32, shape, axis)


def onehot(match):
    return jnp.where(match, 1.0, 0.0).astype(BF16)


def mm(a, b):
    return jnp.dot(a, b, preferred_element_type=F32)


class Plan:
    def __init__(self, tp, hidden, extra):
        self.tp = tp
        self.pair = 2 if tp % 2 == 0 else 1
        self.groups = tp // self.pair
        self.hidden, self.extra = hidden, extra
        self.rows = ceil_to(-(-hidden // LANES), 8)
        self.bins = tp * self.rows
        self.key_span = 1 << max(hidden - 1, 1).bit_length()
        self.slots = min(ceil_to(hidden * 49 // 128, 16), ceil_to(hidden, 16))


def index_kernel(plan, map_ref, slab_ref, key_ref, send_ref, count_ref, top_ref, rank_ref, hist_ref):
    tp, pair, groups, hidden, extra = plan.tp, plan.pair, plan.groups, plan.hidden, plan.extra
    rows, bins = plan.rows, plan.bins
    me = lax.axis_index("tp")
    group = me // pair
    own_low = me - group * pair
    units = map_ref[...]
    block = jnp.zeros_like(units)
    for edge in range(1, tp):
        block += jnp.where(units >= edge * hidden, 1, 0)
    inner = units - block * hidden
    high = block * rows + lax.shift_right_logical(inner, 7)
    low = inner & (LANES - 1)
    total = jnp.ones((bins, LANES), F32)
    for g in range(groups):
        hist = jnp.zeros((bins, LANES), F32)
        for q in range(g * pair, (g + 1) * pair):
            a = onehot(iota((bins, extra), 0) == high[q : q + 1])
            b = onehot(iota((LANES, extra), 0) == low[q : q + 1])
            hist += lax.dot_general(a, b, (((1,), (1,)), ((), ())), preferred_element_type=F32)
        total += hist
        hist_ref[g] = hist
    rank_ref[0] = total
    count_ref[...] = rank_ref[0, pl.ds(me * rows, rows), :]

    bin_row = iota((bins, LANES), 0)
    bin_block = jnp.zeros((bins, LANES), I32)
    for edge in range(1, tp):
        bin_block += jnp.where(bin_row >= edge * rows, 1, 0)
    upper = onehot(iota((LANES, LANES), 0) < iota((LANES, LANES), 1))
    every = jnp.ones((LANES, LANES), BF16)
    row_a, row_b = iota((bins, bins), 0), iota((bins, bins), 1)
    same = jnp.ones((bins, bins), jnp.bool_)
    for edge in range(1, tp):
        same = same & ((row_a >= edge * rows) == (row_b >= edge * rows))
    above = onehot(same & (row_b < row_a))

    def ranks(g):
        named = hist_ref[g] > 0.5
        flags = onehot(named)
        rank = mm(flags, upper) + mm(above, mm(flags, every).astype(BF16))
        return named, rank

    most = jnp.zeros((bins, LANES), F32)
    for g in range(groups):
        named, rank = ranks(g)
        away = (bin_block < g * pair) | (bin_block >= (g + 1) * pair)
        most = jnp.maximum(most, jnp.where(named & away, rank + 1.0, 0.0))
        rank_ref[g] = rank
    top_ref[0] = jnp.max(most).astype(I32)

    for d in range(1, groups):
        target = lax.rem(group + d, groups)
        mine = pl.ds(me * rows, rows)
        send_ref[d - 1] = jnp.where(hist_ref[target, mine, :] > 0.5, rank_ref[target, mine, :], -1.0).astype(I32)

    def own_row(value):
        picked = jnp.zeros((1, extra), I32)
        for q in range(tp):
            picked += jnp.where(me == q, value[q : q + 1], 0)
        return picked

    own_block, own_inner, own_high, own_lo = own_row(block), own_row(inner), own_row(high), own_row(low)
    rank = rank_ref[group]
    rank_high = jnp.floor(rank * (1.0 / LANES))
    rank_low = rank - rank_high * LANES
    pick = onehot(iota((bins, extra), 0) == own_high)
    lane_hit = iota((LANES, extra), 0) == own_lo

    def look_up(table):
        spread = mm(table.T.astype(BF16), pick)
        return jnp.sum(jnp.where(lane_hit, spread, 0.0), axis=0, keepdims=True)

    own_rank = (look_up(rank_high) * LANES + look_up(rank_low)).astype(I32)
    source_group = jnp.zeros((1, extra), I32)
    for edge in range(1, groups):
        source_group += jnp.where(own_block >= edge * pair, 1, 0)
    away = group - source_group
    away = jnp.where(away < 0, away + groups, away)
    side = own_block - source_group * pair - own_low
    side = jnp.where(side < 0, side + pair, side)
    key = (away * pair + side) * plan.key_span + jnp.where(away == 0, own_inner, own_rank)
    key_ref[...] = key
    near = side * hidden + own_inner
    far = pair * hidden + ((away - 1) * pair + side) * plan.slots + own_rank
    nothing = pair * hidden + (tp - pair) * plan.slots
    slab_ref[...] = jnp.where(away == 0, near, jnp.where(own_rank < plan.slots, far, nothing))


def make_index(plan, full_map):
    return pl.pallas_call(
        functools.partial(index_kernel, plan),
        out_shape=(
            jax.ShapeDtypeStruct((1, plan.extra), I32),
            jax.ShapeDtypeStruct((1, plan.extra), I32),
            jax.ShapeDtypeStruct((max(plan.groups - 1, 1), plan.rows, LANES), I32),
            jax.ShapeDtypeStruct((plan.rows, LANES), F32),
            jax.ShapeDtypeStruct((1,), I32),
        ),
        in_specs=[pl.BlockSpec(memory_space=pltpu.VMEM)],
        out_specs=(
            pl.BlockSpec(memory_space=pltpu.VMEM),
            pl.BlockSpec(memory_space=pltpu.VMEM),
            pl.BlockSpec(memory_space=pltpu.VMEM),
            pl.BlockSpec(memory_space=pltpu.VMEM),
            pl.BlockSpec(memory_space=pltpu.SMEM),
        ),
        scratch_shapes=[
            pltpu.VMEM((max(plan.groups, 1), plan.bins, LANES), F32),
            pltpu.VMEM((plan.groups, plan.bins, LANES), F32),
        ],
        compiler_params=pltpu.CompilerParams(vmem_limit_bytes=32 << 20),
        name="index",
    )(full_map)


def pack_kernel(plan, base_ref, send_ref, rows_ref, out_ref, pick_ref):
    hidden, slots = plan.hidden, plan.slots
    place = iota((slots, LANES), 0) + base_ref[0]
    for k in range(-(-hidden // LANES)):
        width = min(LANES, hidden - k * LANES)
        hit = onehot(place == send_ref[k : k + 1, :])
        pick_ref[:, k * LANES : k * LANES + width] = hit[:, :width]
    out_ref[...] = mm(pick_ref[...], rows_ref[...]).astype(BF16)


def pack_rows(plan, base, send, rows):
    width = rows.shape[1]
    return pl.pallas_call(
        functools.partial(pack_kernel, plan),
        out_shape=jax.ShapeDtypeStruct((plan.slots, width), BF16),
        in_specs=[
            pl.BlockSpec(memory_space=pltpu.SMEM),
            pl.BlockSpec(memory_space=pltpu.VMEM),
            pl.BlockSpec(memory_space=pltpu.VMEM),
        ],
        out_specs=pl.BlockSpec(memory_space=pltpu.VMEM),
        scratch_shapes=[pltpu.VMEM((plan.slots, plan.hidden), BF16)],
        compiler_params=pltpu.CompilerParams(vmem_limit_bytes=32 << 20),
        cost_estimate=pl.CostEstimate(
            flops=2 * plan.slots * plan.hidden * width, bytes_accessed=2 * width * (plan.hidden + plan.slots), transcendentals=0
        ),
        name="pack",
    )(base, send, rows)


def spread_kernel(offsets, with_base, base_ref, key_ref, *refs):
    tables = refs[: len(offsets)]
    out_ref, pick_ref = refs[-2:]
    key = key_ref[...]
    total = refs[len(offsets)][...].astype(F32) if with_base else None
    lane = iota(key.shape, 1)
    for table, offset in zip(tables, offsets):
        height = table.shape[0]
        local = key - (offset + base_ref[0])
        for start in range(0, height, LANES):
            width = min(LANES, height - start)
            pick_ref[:, start : start + width] = onehot(local == lane + start)[:, :width]
        part = mm(pick_ref[:, :height], table[...])
        total = part if total is None else total + part
    out_ref[...] = total.astype(BF16)


def spread_rows(base, key, tables, offsets, running, tiles):
    extra, width = key.shape[0], tables[0].shape[1]
    tile = extra // tiles
    with_base = running is not None
    specs = [pl.BlockSpec(memory_space=pltpu.SMEM), pl.BlockSpec((tile, LANES), lambda i: (i, 0))]
    specs += [pl.BlockSpec(memory_space=pltpu.VMEM) for table in tables]
    args = [base, key, *tables]
    aliases = {}
    if with_base:
        specs.append(pl.BlockSpec((tile, width), lambda i: (i, 0)))
        args.append(running)
        aliases = {len(args) - 1: 0}
    depth = sum(t.shape[0] for t in tables)
    return pl.pallas_call(
        functools.partial(spread_kernel, offsets, with_base),
        grid=(tiles,),
        out_shape=jax.ShapeDtypeStruct((extra, width), BF16),
        in_specs=specs,
        out_specs=pl.BlockSpec((tile, width), lambda i: (i, 0)),
        scratch_shapes=[pltpu.VMEM((tile, max(t.shape[0] for t in tables)), BF16)],
        input_output_aliases=aliases,
        compiler_params=pltpu.CompilerParams(vmem_limit_bytes=40 << 20),
        cost_estimate=pl.CostEstimate(
            flops=2 * extra * depth * width, bytes_accessed=2 * width * (extra + depth), transcendentals=0
        ),
        name="spread",
    )(*args)


def column_kernel(key_ref, out_ref):
    extra = key_ref.shape[1]
    key = key_ref[...]
    for start in range(0, extra, LANES):
        width = min(LANES, extra - start)
        out_ref[start : start + width, :] = jnp.broadcast_to(key[:, start : start + width], (LANES, width)).T


def as_column(key):
    return pl.pallas_call(
        column_kernel,
        out_shape=jax.ShapeDtypeStruct((key.shape[1], LANES), I32),
        in_specs=[pl.BlockSpec(memory_space=pltpu.VMEM)],
        out_specs=pl.BlockSpec(memory_space=pltpu.VMEM),
        name="column",
    )(key)


UNROLL = 16


def collect_kernel(lanes, slab_ref, *refs):
    tables, (out_ref, table_ref, stage_ref) = refs[:-3], refs[-3:]
    extra, width = out_ref.shape
    parts = width // lanes
    base = 0
    for table in tables:
        height = table.shape[0]
        chunk = max(c for c in (64, 32, 16, 8, 1) if height % c == 0)

        def widen(i, carry, table=table, base=base, chunk=chunk):
            start = pl.multiple_of(i * chunk, chunk)
            block = table[pl.ds(start, chunk), :].astype(F32)
            for c in range(parts):
                target = (base + start) * parts + c
                table_ref[pl.ds(target, chunk, parts), :] = block[:, c * lanes : (c + 1) * lanes]
            return carry

        lax.fori_loop(0, height // chunk, widen, 0)
        base += height
    table_ref[pl.ds(base * parts, parts), :] = jnp.zeros((parts, lanes), F32)

    unroll = max(u for u in (UNROLL, 8, 4, 2, 1) if extra % u == 0)

    def fetch(i, carry):
        for u in range(unroll):
            j = i * unroll + u
            source = slab_ref[0, j] * parts
            stage_ref[pl.ds(j * parts, parts), :] = table_ref[pl.ds(source, parts), :]
        return carry

    lax.fori_loop(0, extra // unroll, fetch, 0)
    chunk = max(c for c in (64, 32, 16, 8, 1) if extra % c == 0)

    def narrow(i, carry):
        start = pl.multiple_of(i * chunk, chunk)
        for c in range(parts):
            block = stage_ref[pl.ds(start * parts + c, chunk, parts), :]
            out_ref[pl.ds(start, chunk), c * lanes : (c + 1) * lanes] = block.astype(BF16)
        return carry

    lax.fori_loop(0, extra // chunk, narrow, 0)


def collect_rows(slab, tables):
    extra, width = slab.shape[1], tables[0].shape[1]
    lanes = min(width, LANES)
    parts = width // lanes
    depth = sum(t.shape[0] for t in tables)
    return pl.pallas_call(
        functools.partial(collect_kernel, lanes),
        out_shape=jax.ShapeDtypeStruct((extra, width), BF16),
        in_specs=[pl.BlockSpec(memory_space=pltpu.SMEM)] + [pl.BlockSpec(memory_space=pltpu.VMEM) for table in tables],
        out_specs=pl.BlockSpec(memory_space=pltpu.VMEM),
        scratch_shapes=[
            pltpu.VMEM(((depth + 8) * parts, lanes), F32),
            pltpu.VMEM((extra * parts, lanes), F32),
        ],
        compiler_params=pltpu.CompilerParams(vmem_limit_bytes=48 << 20),
        cost_estimate=pl.CostEstimate(
            flops=20 * extra * depth * width // 16, bytes_accessed=2 * width * (extra + depth), transcendentals=0
        ),
        name="collect",
    )(slab, *tables)


def tile_count(extra):
    for tiles in (4, 2):
        if extra % (tiles * 8) == 0:
            return tiles
    return 1


def on_device(gate_weight, up_weight, down_weight, source_map):
    tp = lax.axis_size("tp")
    everyone = tp * lax.axis_size("fsdp")
    share = source_map.shape[0]
    hidden = gate_weight.shape[1]
    extra = share * everyone // tp
    plan = Plan(tp, hidden, extra)
    pair, groups, slots, span = plan.pair, plan.groups, plan.slots, plan.key_span
    tiles = tile_count(extra)
    gate, up = gate_weight.T, up_weight.T

    def swap(rows):
        if pair == 1:
            return []
        return [lax.ppermute(rows, "tp", [(i, i ^ 1) for i in range(tp)])]

    gate_local = [gate] + swap(gate)
    up_local = [up] + swap(up)
    copies = jnp.broadcast_to(source_map[None], (everyone, share))
    full_map = lax.all_to_all(copies, ("fsdp", "tp"), 0, 0, tiled=True)
    slab, key, send, counts, top = make_index(plan, full_map.reshape(tp, extra))
    counts = counts.reshape(-1)[:hidden]
    zero = jnp.zeros((1,), I32)

    def across(base, rows):
        got = []
        for d in range(1, groups):
            packed = pack_rows(plan, base, send[d - 1], rows)
            here = lax.ppermute(packed, "tp", [(i, (i + d * pair) % tp) for i in range(tp)])
            got += [here] + swap(here)
        return got

    def collect(local, remote):
        return collect_rows(slab, local + remote)

    far = tuple(s * span for s in range(pair, tp))
    gate_far = across(zero, gate)
    up_far = across(zero, up)
    kept_down = (down_weight.astype(F32) / counts[:, None]).astype(BF16)
    down_far = across(zero, kept_down)
    down_local = [kept_down] + swap(kept_down)
    grown = [collect(gate_local, gate_far), collect(up_local, up_far), collect(down_local, down_far)]
    if groups > 1:

        def more(state):
            return state[0] * slots < top[0]

        def again(state):
            base = jnp.full((1,), state[0] * slots, I32)
            column = as_column(key)
            out = []
            for rows, running in zip((gate, up, kept_down), state[1:]):
                out.append(spread_rows(base, column, across(base, rows), far, running, tiles))
            return (state[0] + 1, *out)

        _, *grown = lax.while_loop(more, again, (jnp.int32(1), *grown))
    return (grown[0].T, grown[1].T, kept_down, grown[2])


def solution(mesh):
    return jax.shard_map(
        on_device,
        mesh=mesh,
        in_specs=(P("fsdp", "tp"), P("fsdp", "tp"), P("tp", "fsdp"), P(("fsdp", "tp"))),
        out_specs=(P("fsdp", "tp"), P("fsdp", "tp"), P("tp", "fsdp"), P("tp", "fsdp")),
        check_vma=False,
    )
```

```python
import functools
import math

import jax
import jax.numpy as jnp
from jax import lax
from jax.experimental import pallas as pl
from jax.experimental.pallas import tpu as pltpu
from jax.sharding import PartitionSpec as P


LANES = 128
UNIT = 64
F32, BF16, I32 = jnp.float32, jnp.bfloat16, jnp.int32


def ceil_to(value, unit):
    return -(-value // unit) * unit


def iota(shape, axis):
    return lax.broadcasted_iota(I32, shape, axis)


def onehot(match):
    return jnp.where(match, 1.0, 0.0).astype(BF16)


def mm(a, b):
    return jnp.dot(a, b, preferred_element_type=F32)


class Plan:
    def __init__(self, tp, hidden, extra, width):
        self.tp = tp
        self.pair = 2 if tp % 2 == 0 else 1
        self.groups = tp // self.pair
        self.hidden, self.extra = hidden, extra
        self.rows = ceil_to(-(-hidden // LANES), 8)
        self.bins = tp * self.rows
        self.lanes = min(width, LANES)
        self.parts = width // self.lanes
        self.halves = 2 if self.parts % 2 == 0 else 1
        self.slots = max(hidden * 3 // 8 // UNIT * UNIT, min(UNIT, hidden))
        self.rest = hidden - self.slots
        self.head = min(ceil_to(self.slots // 4, UNIT), self.slots)


def split_units(plan, units):
    block = jnp.zeros_like(units)
    for edge in range(1, plan.tp):
        block += jnp.where(units >= edge * plan.hidden, 1, 0)
    inner = units - block * plan.hidden
    high = block * plan.rows + lax.shift_right_logical(inner, 7)
    return block, inner, high, inner & (LANES - 1)


def index_kernel(plan, map_ref, gate_ref, own_ref, send_ref, count_ref, top_ref, *refs):
    head_refs, (rank_ref, hist_ref, rows_ref, pick_ref, sem) = refs[:-5], refs[-5:]
    gate_copy = pltpu.make_async_copy(gate_ref, rows_ref, sem)
    gate_copy.start()
    tp, pair, groups, extra = plan.tp, plan.pair, plan.groups, plan.extra
    rows, bins = plan.rows, plan.bins
    me = lax.axis_index("tp")
    group = me // pair
    _, _, high, low = split_units(plan, map_ref[...])
    total = jnp.ones((bins, LANES), F32)
    for g in range(groups):
        hist = jnp.zeros((bins, LANES), F32)
        for q in range(g * pair, (g + 1) * pair):
            a = onehot(iota((bins, extra), 0) == high[q : q + 1])
            b = onehot(iota((LANES, extra), 0) == low[q : q + 1])
            hist += lax.dot_general(a, b, (((1,), (1,)), ((), ())), preferred_element_type=F32)
        total += hist
        hist_ref[g] = hist
    rank_ref[0] = total
    count_ref[...] = rank_ref[0, pl.ds(me * rows, rows), :]

    bin_row = iota((bins, LANES), 0)
    bin_block = jnp.zeros((bins, LANES), I32)
    for edge in range(1, tp):
        bin_block += jnp.where(bin_row >= edge * rows, 1, 0)
    upper = onehot(iota((LANES, LANES), 0) < iota((LANES, LANES), 1))
    every = jnp.ones((LANES, LANES), BF16)
    row_a, row_b = iota((bins, bins), 0), iota((bins, bins), 1)
    same = jnp.ones((bins, bins), jnp.bool_)
    for edge in range(1, tp):
        same = same & ((row_a >= edge * rows) == (row_b >= edge * rows))
    above = onehot(same & (row_b < row_a))

    def ranks(g):
        named = hist_ref[g] > 0.5
        flags = onehot(named)
        rank = mm(flags, upper) + mm(above, mm(flags, every).astype(BF16))
        return named, rank

    most = jnp.zeros((bins, LANES), F32)
    for g in range(groups):
        named, rank = ranks(g)
        away = (bin_block < g * pair) | (bin_block >= (g + 1) * pair)
        most = jnp.maximum(most, jnp.where(named & away, rank + 1.0, 0.0))
        rank_ref[g] = rank
    top_ref[0] = jnp.max(most).astype(I32)

    for d in range(1, groups):
        target = lax.rem(group + d, groups)
        mine = pl.ds(me * rows, rows)
        send_ref[d - 1] = jnp.where(hist_ref[target, mine, :] > 0.5, rank_ref[target, mine, :], -1.0).astype(I32)

    own_ref[...] = rank_ref[group]
    gate_copy.wait()
    for d, head_ref in enumerate(head_refs):
        box = (0, plan.head, 0, gate_ref.shape[1])
        pack_kernel(plan, [box], send_ref.at[d], rows_ref, head_ref, pick_ref)


def keys_kernel(plan, map_ref, rank_ref, slab_ref, half_ref):
    tp, pair, groups, hidden, extra, bins = plan.tp, plan.pair, plan.groups, plan.hidden, plan.extra, plan.bins
    me = lax.axis_index("tp")
    group = me // pair
    own_low = me - group * pair
    units = map_ref[...]
    own = jnp.zeros((1, extra), I32)
    for q in range(tp):
        own += jnp.where(me == q, units[q : q + 1], 0)
    own_block, own_inner, own_high, own_lo = split_units(plan, own)
    rank = rank_ref[...]
    rank_high = jnp.floor(rank * (1.0 / LANES))
    rank_low = rank - rank_high * LANES
    pick = onehot(iota((bins, extra), 0) == own_high)
    lane_hit = iota((LANES, extra), 0) == own_lo

    def look_up(table):
        spread = mm(table.T.astype(BF16), pick)
        return jnp.sum(jnp.where(lane_hit, spread, 0.0), axis=0, keepdims=True)

    own_rank = (look_up(rank_high) * LANES + look_up(rank_low)).astype(I32)
    source_group = jnp.zeros((1, extra), I32)
    for edge in range(1, groups):
        source_group += jnp.where(own_block >= edge * pair, 1, 0)
    away = group - source_group
    away = jnp.where(away < 0, away + groups, away)
    side = own_block - source_group * pair - own_low
    side = jnp.where(side < 0, side + pair, side)
    near = side * hidden + own_inner
    sides = tp - pair
    table = (away - 1) * pair + side
    first = pair * hidden + table * plan.slots + own_rank
    later = pair * hidden + sides * plan.slots + table * plan.rest + own_rank - plan.slots
    row = jnp.where(away == 0, near, jnp.where(own_rank < plan.slots, first, later))
    slab_ref[...] = row * plan.parts
    half_ref[...] = row * (plan.parts // plan.halves)


def make_index(plan, full_map, gate):
    others = plan.groups - 1
    vmem, smem = pl.BlockSpec(memory_space=pltpu.VMEM), pl.BlockSpec(memory_space=pltpu.SMEM)
    head = jax.ShapeDtypeStruct((plan.head, gate.shape[1]), BF16)
    return pl.pallas_call(
        functools.partial(index_kernel, plan),
        out_shape=[
            jax.ShapeDtypeStruct((plan.bins, LANES), F32),
            jax.ShapeDtypeStruct((max(others, 1), plan.rows, LANES), I32),
            jax.ShapeDtypeStruct((plan.rows, LANES), F32),
            jax.ShapeDtypeStruct((1,), I32),
        ]
        + [head] * others,
        in_specs=[vmem, pl.BlockSpec(memory_space=pltpu.HBM)],
        out_specs=[vmem, vmem, vmem, smem] + [vmem] * others,
        scratch_shapes=[
            pltpu.VMEM((plan.groups, plan.bins, LANES), F32),
            pltpu.VMEM((plan.groups, plan.bins, LANES), F32),
            pltpu.VMEM(gate.shape, BF16),
            pltpu.VMEM((plan.head, plan.hidden), BF16),
            pltpu.SemaphoreType.DMA,
        ],
        compiler_params=pltpu.CompilerParams(vmem_limit_bytes=32 << 20),
        name="index",
    )(full_map, gate)


def make_keys(plan, full_map, rank):
    vmem = pl.BlockSpec(memory_space=pltpu.VMEM)
    return pl.pallas_call(
        functools.partial(keys_kernel, plan),
        out_shape=[jax.ShapeDtypeStruct((1, plan.extra), I32)] * 2,
        in_specs=[vmem, vmem],
        out_specs=[vmem, vmem],
        compiler_params=pltpu.CompilerParams(vmem_limit_bytes=24 << 20),
        name="keys",
    )(full_map, rank)


def pack_kernel(plan, boxes, send_ref, rows_ref, *refs):
    hidden = plan.hidden
    out_refs, pick_ref = refs[:-1], refs[-1]
    first = boxes[0][0]
    place = iota((pick_ref.shape[0], LANES), 0) + first
    for k in range(-(-hidden // LANES)):
        width = min(LANES, hidden - k * LANES)
        hit = onehot(place == send_ref[k : k + 1, :])
        pick_ref[:, k * LANES : k * LANES + width] = hit[:, :width]
    for out_ref, (top, bottom, left, right) in zip(out_refs, boxes):
        out_ref[...] = mm(pick_ref[top - first : bottom - first, :], rows_ref[:, left:right]).astype(BF16)


def pack_rows(plan, send, rows, boxes):
    width = rows.shape[1]
    total = max(box[1] for box in boxes) - boxes[0][0]
    return pl.pallas_call(
        functools.partial(pack_kernel, plan, boxes),
        out_shape=[jax.ShapeDtypeStruct((b - a, d - c), BF16) for a, b, c, d in boxes],
        in_specs=[pl.BlockSpec(memory_space=pltpu.VMEM), pl.BlockSpec(memory_space=pltpu.VMEM)],
        out_specs=[pl.BlockSpec(memory_space=pltpu.VMEM) for box in boxes],
        scratch_shapes=[pltpu.VMEM((total, plan.hidden), BF16)],
        compiler_params=pltpu.CompilerParams(vmem_limit_bytes=(24 if total <= plan.slots else 48) << 20),
        cost_estimate=pl.CostEstimate(
            flops=2 * total * plan.hidden * width, bytes_accessed=2 * width * (plan.hidden + total), transcendentals=0
        ),
        name="pack",
    )(send, rows)


def nothing_kernel(*refs):
    pass


def unwritten(shape):
    return pl.pallas_call(
        nothing_kernel,
        out_shape=jax.ShapeDtypeStruct(shape, BF16),
        out_specs=pl.BlockSpec(memory_space=pltpu.HBM),
        compiler_params=pltpu.CompilerParams(has_side_effects=True),
        name="room",
    )()


UNROLL = 64


def chunk_of(height):
    return max(c for c in (96, 64, 48, 32, 16, 8, 4, 2, 1) if height % c == 0)


def pieces_of(height):
    chunk = chunk_of(height)
    if height < 1500:
        return [(0, height)]
    size = ceil_to(height // chunk, 4) // 4 * chunk
    return [(start, min(size, height - start)) for start in range(0, height, size)]


def collect_kernel(plan, half, counts, top_ref, slab_ref, *refs):
    resident, always, later = counts
    tables, refs = refs[: always + later], refs[always + later :]
    out_ref, land_ref, table_ref, stage_ref, ready_ref, in_sems, out_sems = refs[-7:]
    extra, width = ready_ref.shape
    lanes = plan.lanes
    parts = width // lanes
    columns = pl.ds(half * width, width)
    fixed = slice(half * width, (half + 1) * width)
    starts = [0]
    for table in tables:
        starts.append(starts[-1] + table.shape[0])
    landed = {}
    for i in range(always + later):
        if i not in resident:
            landed[i] = sum(tables[k].shape[0] for k in landed)

    def load(which, first):
        loads = []
        for i in which:
            table = tables[i]
            whole = table.shape[1] == width
            for start, size in pieces_of(table.shape[0]):
                rows = pl.ds(start, size)
                land = landed[i] + start
                source = table.at[rows] if whole else table.at[rows, columns]
                copy = pltpu.make_async_copy(source, land_ref.at[pl.ds(land, size)], in_sems.at[first + len(loads)])
                copy.start()
                loads.append((copy, starts[i] + start, land, size))
        return loads

    def widen(source, at, begin, size, cut):
        chunk = chunk_of(size)

        def step(i, carry):
            start = pl.multiple_of(at + i * chunk, math.gcd(at, chunk))
            block = source[pl.ds(start, chunk), cut].astype(F32)
            for c in range(parts):
                target = (begin + i * chunk) * parts + c
                table_ref[pl.ds(target, chunk, parts), :] = block[:, c * lanes : (c + 1) * lanes]
            return carry

        lax.fori_loop(0, size // chunk, step, 0)

    def widen_all(loads):
        for copy, begin, land, size in loads:
            copy.wait()
            widen(land_ref, land, begin, size, slice(None))

    loads = load([i for i in range(always) if i not in resident], 0)
    for i in resident:
        cut = slice(None) if tables[i].shape[1] == width else fixed
        widen(tables[i], 0, starts[i], tables[i].shape[0], cut)
    widen_all(loads)
    if later:

        @pl.when(top_ref[0] > plan.slots)
        def _():
            widen_all(load(range(always, always + later), len(loads)))

    stores = []
    for piece, (begin, size) in enumerate(pieces_of(extra)):
        unroll = max(u for u in (UNROLL, 32, 16, 8, 4, 2, 1) if size % u == 0)
        chunk = chunk_of(size)

        def fetch(i, carry, begin=begin, unroll=unroll):
            for u in range(unroll):
                j = begin + i * unroll + u
                source = pl.multiple_of(slab_ref[0, j], parts)
                stage_ref[pl.ds(j * parts, parts), :] = table_ref[pl.ds(source, parts), :]
            return carry

        lax.fori_loop(0, size // unroll, fetch, 0)

        def narrow(i, carry, begin=begin, chunk=chunk):
            start = pl.multiple_of(begin + i * chunk, math.gcd(begin, chunk))
            for c in range(parts):
                block = stage_ref[pl.ds(start * parts + c, chunk, parts), :]
                ready_ref[pl.ds(start, chunk), c * lanes : (c + 1) * lanes] = block.astype(BF16)
            return carry

        lax.fori_loop(0, size // chunk, narrow, 0)
        part = pl.ds(begin, size)
        target = out_ref.at[part] if out_ref.shape[1] == width else out_ref.at[part, columns]
        copy = pltpu.make_async_copy(ready_ref.at[part], target, out_sems.at[piece])
        copy.start()
        stores.append(copy)
    for copy in stores:
        copy.wait()


def collect_rows(plan, top, slab, tables, resident, spare, half=0, halves=1, running=None):
    extra, full = plan.extra, tables[0].shape[1]
    width = full // halves
    lanes = plan.lanes
    parts = width // lanes
    depth = sum(t.shape[0] for t in tables + spare)
    landing = [t for i, t in enumerate(tables) if i not in resident] + spare
    loads = sum(len(pieces_of(t.shape[0])) for t in landing)
    landed = sum(t.shape[0] for t in landing)
    vmem = pl.BlockSpec(memory_space=pltpu.VMEM)
    smem, hbm = pl.BlockSpec(memory_space=pltpu.SMEM), pl.BlockSpec(memory_space=pltpu.HBM)
    held = [pltpu.with_memory_space_constraint(t, pltpu.VMEM) if i in resident else t for i, t in enumerate(tables)]
    specs = [vmem if i in resident else hbm for i in range(len(tables))] + [hbm] * len(spare)
    args = [top, slab, *held, *spare]
    aliases = {}
    if running is not None:
        aliases = {len(args): 0}
        specs.append(hbm)
        args.append(running)
    return pl.pallas_call(
        functools.partial(collect_kernel, plan, half, (resident, len(tables), len(spare))),
        out_shape=jax.ShapeDtypeStruct((extra, full), BF16),
        in_specs=[smem, smem] + specs,
        out_specs=hbm,
        scratch_shapes=[
            pltpu.VMEM((landed, width), BF16),
            pltpu.VMEM((depth * parts, lanes), F32),
            pltpu.VMEM((extra * parts, lanes), F32),
            pltpu.VMEM((extra, width), BF16),
            pltpu.SemaphoreType.DMA((loads,)),
            pltpu.SemaphoreType.DMA((len(pieces_of(extra)),)),
        ],
        input_output_aliases=aliases,
        compiler_params=pltpu.CompilerParams(vmem_limit_bytes=(45 if halves == 1 else 25) << 20),
        cost_estimate=pl.CostEstimate(
            flops=20 * extra * depth * width // 16, bytes_accessed=2 * width * (extra + depth), transcendentals=0
        ),
        name="collect",
    )(*args)


def on_device(gate_weight, up_weight, down_weight, source_map):
    tp = lax.axis_size("tp")
    everyone = tp * lax.axis_size("fsdp")
    share = source_map.shape[0]
    hidden = gate_weight.shape[1]
    extra = share * everyone // tp
    plan = Plan(tp, hidden, extra, gate_weight.shape[0])
    pair, groups, slots = plan.pair, plan.groups, plan.slots
    gate, up = gate_weight.T, up_weight.T

    def swap(rows):
        if pair == 1:
            return []
        return [lax.ppermute(rows, "tp", [(i, i ^ 1) for i in range(tp)])]


    copies = jnp.broadcast_to(source_map[None], (everyone, share))
    full_map = lax.all_to_all(copies, ("fsdp", "tp"), 0, 0, tiled=True)
    full_map = full_map.reshape(tp, extra)
    rank, send, counts, top, *heads = make_index(plan, full_map, gate)
    slab, half_slab = make_keys(plan, full_map, rank)
    counts = counts.reshape(-1)[:hidden]

    def wire(rows, d):
        return lax.ppermute(rows, "tp", [(i, (i + d * pair) % tp) for i in range(tp)])

    width = gate_weight.shape[0]

    def across(rows, groups_of_boxes, ready=()):
        sides = []
        for d in range(1, groups):
            packed = list(ready[d - 1 : d])
            for boxes in groups_of_boxes:
                packed += pack_rows(plan, send[d - 1], rows, boxes)
            here = [wire(part, d) for part in packed]
            there = [swap(part) for part in here]
            sides += [here] + [list(side) for side in zip(*there)]
        return sides

    def flat(sides):
        return [part for side in sides for part in side]

    def collect(slab, local, sides, spare, **more):
        tables = local + flat(sides)
        at, resident = len(local), []
        for i, side in enumerate(sides):
            resident += range(at, at + len(side)) if i % pair else []
            at += len(side)
        return collect_rows(plan, top, slab, tables, resident, spare, **more)

    halves = plan.halves
    column = width // halves
    gate_local = [gate] + swap(gate)
    up_local = [up] + swap(up)
    gate_far = across(gate, [[(plan.head, slots, 0, width)]], heads)
    up_far = across(up, [[(0, slots, 0, width)]])
    kept_down = (down_weight.astype(F32) / counts[:, None]).astype(BF16)
    down_boxes = [(0, slots, h * column, (h + 1) * column) for h in range(halves)]
    down_far = across(kept_down, [down_boxes])
    down_local = [kept_down] + swap(kept_down)
    spare = [[], [], []]
    if groups > 1 and plan.rest > 0:
        sides = tp - pair
        rooms = tuple(unwritten((plan.rest, width)) for _ in range(3 * sides))

        def again(state):
            filled = []
            for rows in (gate, up, kept_down):
                filled += flat(across(rows, [[(slots, hidden, 0, width)]]))
            return (jnp.bool_(False), *filled)

        _, *rooms = lax.while_loop(lambda state: state[0], again, (top[0] > slots, *rooms))
        spare = [rooms[i * sides : (i + 1) * sides] for i in range(3)]
    added_gate = collect(slab, gate_local, gate_far, spare[0])
    added_up = collect(slab, up_local, up_far, spare[1])
    added_down = None
    for h in range(halves):
        sides = [[side[h]] for side in down_far]
        added_down = collect(
            half_slab, down_local, sides, spare[2], half=h, halves=halves, running=added_down
        )
    return (added_gate.T, added_up.T, kept_down, added_down)


def solution(mesh):
    return jax.shard_map(
        on_device,
        mesh=mesh,
        in_specs=(P("fsdp", "tp"), P("fsdp", "tp"), P("tp", "fsdp"), P(("fsdp", "tp"))),
        out_specs=(P("fsdp", "tp"), P("fsdp", "tp"), P("tp", "fsdp"), P("tp", "fsdp")),
        check_vma=False,
    )
```

```python
import functools
import math

import jax
import jax.numpy as jnp
from jax import lax
from jax.experimental import pallas as pl
from jax.experimental.pallas import tpu as pltpu
from jax.sharding import PartitionSpec as P


LANES = 128
UNIT = 64
F32, BF16, I32 = jnp.float32, jnp.bfloat16, jnp.int32


def ceil_to(value, unit):
    return -(-value // unit) * unit


def iota(shape, axis):
    return lax.broadcasted_iota(I32, shape, axis)


def onehot(match):
    return jnp.where(match, 1.0, 0.0).astype(BF16)


def mm(a, b):
    return jnp.dot(a, b, preferred_element_type=F32)


class Plan:
    def __init__(self, tp, hidden, extra, width):
        self.tp = tp
        self.pair = 2 if tp % 2 == 0 else 1
        self.groups = tp // self.pair
        self.hidden, self.extra = hidden, extra
        self.rows = ceil_to(-(-hidden // LANES), 8)
        self.bins = tp * self.rows
        self.lanes = min(width, LANES)
        self.parts = width // self.lanes
        self.halves = 2 if self.parts % 2 == 0 else 1
        self.slots = max(hidden * 3 // 8 // UNIT * UNIT, min(UNIT, hidden))
        self.rest = hidden - self.slots
        self.head = min(ceil_to(self.slots // 4, UNIT), self.slots)


def split_units(plan, units):
    block = jnp.zeros_like(units)
    for edge in range(1, plan.tp):
        block += jnp.where(units >= edge * plan.hidden, 1, 0)
    inner = units - block * plan.hidden
    high = block * plan.rows + lax.shift_right_logical(inner, 7)
    return block, inner, high, inner & (LANES - 1)


def index_kernel(plan, map_ref, gate_ref, own_ref, send_ref, count_ref, top_ref, *refs):
    head_refs, (rank_ref, hist_ref, units_ref, rows_ref, pick_ref, sems) = refs[:-6], refs[-6:]
    map_copy = pltpu.make_async_copy(map_ref, units_ref, sems.at[0])
    gate_copy = pltpu.make_async_copy(gate_ref, rows_ref, sems.at[1])
    map_copy.start()
    gate_copy.start()
    map_copy.wait()
    tp, pair, groups, extra = plan.tp, plan.pair, plan.groups, plan.extra
    rows, bins = plan.rows, plan.bins
    me = lax.axis_index("tp")
    group = me // pair
    _, _, high, low = split_units(plan, units_ref[...])
    total = jnp.ones((bins, LANES), F32)
    for g in range(groups):
        hist = jnp.zeros((bins, LANES), F32)
        for q in range(g * pair, (g + 1) * pair):
            a = onehot(iota((bins, extra), 0) == high[q : q + 1])
            b = onehot(iota((LANES, extra), 0) == low[q : q + 1])
            hist += lax.dot_general(a, b, (((1,), (1,)), ((), ())), preferred_element_type=F32)
        total += hist
        hist_ref[g] = hist
    rank_ref[0] = total
    count_ref[...] = rank_ref[0, pl.ds(me * rows, rows), :]

    bin_row = iota((bins, LANES), 0)
    bin_block = jnp.zeros((bins, LANES), I32)
    for edge in range(1, tp):
        bin_block += jnp.where(bin_row >= edge * rows, 1, 0)
    upper = onehot(iota((LANES, LANES), 0) < iota((LANES, LANES), 1))
    every = jnp.ones((LANES, LANES), BF16)
    row_a, row_b = iota((bins, bins), 0), iota((bins, bins), 1)
    same = jnp.ones((bins, bins), jnp.bool_)
    for edge in range(1, tp):
        same = same & ((row_a >= edge * rows) == (row_b >= edge * rows))
    above = onehot(same & (row_b < row_a))

    def ranks(g):
        named = hist_ref[g] > 0.5
        flags = onehot(named)
        rank = mm(flags, upper) + mm(above, mm(flags, every).astype(BF16))
        return named, rank

    most = jnp.zeros((bins, LANES), F32)
    for g in range(groups):
        named, rank = ranks(g)
        away = (bin_block < g * pair) | (bin_block >= (g + 1) * pair)
        most = jnp.maximum(most, jnp.where(named & away, rank + 1.0, 0.0))
        rank_ref[g] = rank
    top_ref[0] = jnp.max(most).astype(I32)

    for d in range(1, groups):
        target = lax.rem(group + d, groups)
        mine = pl.ds(me * rows, rows)
        send_ref[d - 1] = jnp.where(hist_ref[target, mine, :] > 0.5, rank_ref[target, mine, :], -1.0).astype(I32)

    own_ref[...] = rank_ref[group]
    gate_copy.wait()
    for d, head_ref in enumerate(head_refs):
        box = (0, plan.head, 0, gate_ref.shape[1])
        pack_kernel(plan, [box], send_ref.at[d], rows_ref, head_ref, pick_ref)


def keys_kernel(plan, map_ref, rank_ref, slab_ref, half_ref):
    tp, pair, groups, hidden, extra, bins = plan.tp, plan.pair, plan.groups, plan.hidden, plan.extra, plan.bins
    me = lax.axis_index("tp")
    group = me // pair
    own_low = me - group * pair
    units = map_ref[...]
    own = jnp.zeros((1, extra), I32)
    for q in range(tp):
        own += jnp.where(me == q, units[q : q + 1], 0)
    own_block, own_inner, own_high, own_lo = split_units(plan, own)
    rank = rank_ref[...]
    rank_high = jnp.floor(rank * (1.0 / LANES))
    rank_low = rank - rank_high * LANES
    pick = onehot(iota((bins, extra), 0) == own_high)
    lane_hit = iota((LANES, extra), 0) == own_lo

    def look_up(table):
        spread = mm(table.T.astype(BF16), pick)
        return jnp.sum(jnp.where(lane_hit, spread, 0.0), axis=0, keepdims=True)

    own_rank = (look_up(rank_high) * LANES + look_up(rank_low)).astype(I32)
    source_group = jnp.zeros((1, extra), I32)
    for edge in range(1, groups):
        source_group += jnp.where(own_block >= edge * pair, 1, 0)
    away = group - source_group
    away = jnp.where(away < 0, away + groups, away)
    side = own_block - source_group * pair - own_low
    side = jnp.where(side < 0, side + pair, side)
    near = side * hidden + own_inner
    sides = tp - pair
    table = (away - 1) * pair + side
    first = pair * hidden + table * plan.slots + own_rank
    later = pair * hidden + sides * plan.slots + table * plan.rest + own_rank - plan.slots
    row = jnp.where(away == 0, near, jnp.where(own_rank < plan.slots, first, later))
    slab_ref[...] = row * plan.parts
    half_ref[...] = row * (plan.parts // plan.halves)


def make_index(plan, full_map, gate):
    others = plan.groups - 1
    vmem, smem = pl.BlockSpec(memory_space=pltpu.VMEM), pl.BlockSpec(memory_space=pltpu.SMEM)
    head = jax.ShapeDtypeStruct((plan.head, gate.shape[1]), BF16)
    return pl.pallas_call(
        functools.partial(index_kernel, plan),
        out_shape=[
            jax.ShapeDtypeStruct((plan.bins, LANES), F32),
            jax.ShapeDtypeStruct((max(others, 1), plan.rows, LANES), I32),
            jax.ShapeDtypeStruct((plan.rows, LANES), F32),
            jax.ShapeDtypeStruct((1,), I32),
        ]
        + [head] * others,
        in_specs=[pl.BlockSpec(memory_space=pltpu.HBM)] * 2,
        out_specs=[vmem, vmem, vmem, smem] + [vmem] * others,
        scratch_shapes=[
            pltpu.VMEM((plan.groups, plan.bins, LANES), F32),
            pltpu.VMEM((plan.groups, plan.bins, LANES), F32),
            pltpu.VMEM(full_map.shape, I32),
            pltpu.VMEM(gate.shape, BF16),
            pltpu.VMEM((plan.head, plan.hidden), BF16),
            pltpu.SemaphoreType.DMA((2,)),
        ],
        compiler_params=pltpu.CompilerParams(vmem_limit_bytes=32 << 20),
        name="index",
    )(full_map, gate)


def make_keys(plan, full_map, rank):
    vmem = pl.BlockSpec(memory_space=pltpu.VMEM)
    return pl.pallas_call(
        functools.partial(keys_kernel, plan),
        out_shape=[jax.ShapeDtypeStruct((1, plan.extra), I32)] * 2,
        in_specs=[vmem, vmem],
        out_specs=[vmem, vmem],
        compiler_params=pltpu.CompilerParams(vmem_limit_bytes=24 << 20),
        name="keys",
    )(full_map, rank)


def pack_kernel(plan, boxes, send_ref, rows_ref, *refs):
    hidden = plan.hidden
    out_refs, pick_ref = refs[:-1], refs[-1]
    first = boxes[0][0]
    place = iota((pick_ref.shape[0], LANES), 0) + first
    for k in range(-(-hidden // LANES)):
        width = min(LANES, hidden - k * LANES)
        hit = onehot(place == send_ref[k : k + 1, :])
        pick_ref[:, k * LANES : k * LANES + width] = hit[:, :width]
    for out_ref, (top, bottom, left, right) in zip(out_refs, boxes):
        out_ref[...] = mm(pick_ref[top - first : bottom - first, :], rows_ref[:, left:right]).astype(BF16)


def pack_rows(plan, send, rows, boxes):
    width = rows.shape[1]
    total = max(box[1] for box in boxes) - boxes[0][0]
    return pl.pallas_call(
        functools.partial(pack_kernel, plan, boxes),
        out_shape=[jax.ShapeDtypeStruct((b - a, d - c), BF16) for a, b, c, d in boxes],
        in_specs=[pl.BlockSpec(memory_space=pltpu.VMEM), pl.BlockSpec(memory_space=pltpu.VMEM)],
        out_specs=[pl.BlockSpec(memory_space=pltpu.VMEM) for box in boxes],
        scratch_shapes=[pltpu.VMEM((total, plan.hidden), BF16)],
        compiler_params=pltpu.CompilerParams(vmem_limit_bytes=(24 if total <= plan.slots else 48) << 20),
        cost_estimate=pl.CostEstimate(
            flops=2 * total * plan.hidden * width, bytes_accessed=2 * width * (plan.hidden + total), transcendentals=0
        ),
        name="pack",
    )(send, rows)


def nothing_kernel(*refs):
    pass


def unwritten(shape):
    return pl.pallas_call(
        nothing_kernel,
        out_shape=jax.ShapeDtypeStruct(shape, BF16),
        out_specs=pl.BlockSpec(memory_space=pltpu.HBM),
        compiler_params=pltpu.CompilerParams(has_side_effects=True),
        name="room",
    )()


UNROLL = 64


def chunk_of(height):
    return max(c for c in (96, 64, 48, 32, 16, 8, 4, 2, 1) if height % c == 0)


def pieces_of(height):
    chunk = chunk_of(height)
    if height < 1500:
        return [(0, height)]
    size = ceil_to(height // chunk, 4) // 4 * chunk
    return [(start, min(size, height - start)) for start in range(0, height, size)]


def collect_kernel(plan, half, counts, top_ref, slab_ref, *refs):
    resident, always, later = counts
    tables, refs = refs[: always + later], refs[always + later :]
    out_ref, land_ref, table_ref, stage_ref, ready_ref, in_sems, out_sems = refs[-7:]
    extra, width = ready_ref.shape
    lanes = plan.lanes
    parts = width // lanes
    columns = pl.ds(half * width, width)
    fixed = slice(half * width, (half + 1) * width)
    starts = [0]
    for table in tables:
        starts.append(starts[-1] + table.shape[0])
    landed = {}
    for i in range(always + later):
        if i not in resident:
            landed[i] = sum(tables[k].shape[0] for k in landed)

    def load(which, first):
        loads = []
        for i in which:
            table = tables[i]
            whole = table.shape[1] == width
            for start, size in pieces_of(table.shape[0]):
                rows = pl.ds(start, size)
                land = landed[i] + start
                source = table.at[rows] if whole else table.at[rows, columns]
                copy = pltpu.make_async_copy(source, land_ref.at[pl.ds(land, size)], in_sems.at[first + len(loads)])
                copy.start()
                loads.append((copy, starts[i] + start, land, size))
        return loads

    def widen(source, at, begin, size, cut):
        chunk = chunk_of(size)

        def step(i, carry):
            start = pl.multiple_of(at + i * chunk, math.gcd(at, chunk))
            block = source[pl.ds(start, chunk), cut].astype(F32)
            for c in range(parts):
                target = (begin + i * chunk) * parts + c
                table_ref[pl.ds(target, chunk, parts), :] = block[:, c * lanes : (c + 1) * lanes]
            return carry

        lax.fori_loop(0, size // chunk, step, 0)

    def widen_all(loads):
        for copy, begin, land, size in loads:
            copy.wait()
            widen(land_ref, land, begin, size, slice(None))

    loads = load([i for i in range(always) if i not in resident], 0)
    for i in resident:
        cut = slice(None) if tables[i].shape[1] == width else fixed
        widen(tables[i], 0, starts[i], tables[i].shape[0], cut)
    widen_all(loads)
    if later:

        @pl.when(top_ref[0] > plan.slots)
        def _():
            widen_all(load(range(always, always + later), len(loads)))

    stores = []
    for piece, (begin, size) in enumerate(pieces_of(extra)):
        unroll = max(u for u in (UNROLL, 32, 16, 8, 4, 2, 1) if size % u == 0)
        chunk = chunk_of(size)

        def fetch(i, carry, begin=begin, unroll=unroll):
            for u in range(unroll):
                j = begin + i * unroll + u
                source = pl.multiple_of(slab_ref[0, j], parts)
                stage_ref[pl.ds(j * parts, parts), :] = table_ref[pl.ds(source, parts), :]
            return carry

        lax.fori_loop(0, size // unroll, fetch, 0)

        def narrow(i, carry, begin=begin, chunk=chunk):
            start = pl.multiple_of(begin + i * chunk, math.gcd(begin, chunk))
            for c in range(parts):
                block = stage_ref[pl.ds(start * parts + c, chunk, parts), :]
                ready_ref[pl.ds(start, chunk), c * lanes : (c + 1) * lanes] = block.astype(BF16)
            return carry

        lax.fori_loop(0, size // chunk, narrow, 0)
        part = pl.ds(begin, size)
        target = out_ref.at[part] if out_ref.shape[1] == width else out_ref.at[part, columns]
        copy = pltpu.make_async_copy(ready_ref.at[part], target, out_sems.at[piece])
        copy.start()
        stores.append(copy)
    for copy in stores:
        copy.wait()


def collect_rows(plan, top, slab, tables, resident, spare, half=0, halves=1, running=None):
    extra, full = plan.extra, tables[0].shape[1]
    width = full // halves
    lanes = plan.lanes
    parts = width // lanes
    depth = sum(t.shape[0] for t in tables + spare)
    landing = [t for i, t in enumerate(tables) if i not in resident] + spare
    loads = sum(len(pieces_of(t.shape[0])) for t in landing)
    landed = sum(t.shape[0] for t in landing)
    vmem = pl.BlockSpec(memory_space=pltpu.VMEM)
    smem, hbm = pl.BlockSpec(memory_space=pltpu.SMEM), pl.BlockSpec(memory_space=pltpu.HBM)
    held = [pltpu.with_memory_space_constraint(t, pltpu.VMEM) if i in resident else t for i, t in enumerate(tables)]
    specs = [vmem if i in resident else hbm for i in range(len(tables))] + [hbm] * len(spare)
    args = [top, slab, *held, *spare]
    aliases = {}
    if running is not None:
        aliases = {len(args): 0}
        specs.append(hbm)
        args.append(running)
    return pl.pallas_call(
        functools.partial(collect_kernel, plan, half, (resident, len(tables), len(spare))),
        out_shape=jax.ShapeDtypeStruct((extra, full), BF16),
        in_specs=[smem, smem] + specs,
        out_specs=hbm,
        scratch_shapes=[
            pltpu.VMEM((landed, width), BF16),
            pltpu.VMEM((depth * parts, lanes), F32),
            pltpu.VMEM((extra * parts, lanes), F32),
            pltpu.VMEM((extra, width), BF16),
            pltpu.SemaphoreType.DMA((loads,)),
            pltpu.SemaphoreType.DMA((len(pieces_of(extra)),)),
        ],
        input_output_aliases=aliases,
        compiler_params=pltpu.CompilerParams(vmem_limit_bytes=(45 if halves == 1 else 25) << 20),
        cost_estimate=pl.CostEstimate(
            flops=20 * extra * depth * width // 16, bytes_accessed=2 * width * (extra + depth), transcendentals=0
        ),
        name="collect",
    )(*args)


def on_device(gate_weight, up_weight, down_weight, source_map):
    tp = lax.axis_size("tp")
    everyone = tp * lax.axis_size("fsdp")
    share = source_map.shape[0]
    hidden = gate_weight.shape[1]
    extra = share * everyone // tp
    plan = Plan(tp, hidden, extra, gate_weight.shape[0])
    pair, groups, slots = plan.pair, plan.groups, plan.slots
    gate, up = gate_weight.T, up_weight.T

    def swap(rows):
        if pair == 1:
            return []
        return [lax.ppermute(rows, "tp", [(i, i ^ 1) for i in range(tp)])]


    copies = jnp.broadcast_to(source_map[None], (everyone, share))
    full_map = lax.all_to_all(copies, ("fsdp", "tp"), 0, 0, tiled=True)
    full_map = full_map.reshape(tp, extra)
    rank, send, counts, top, *heads = make_index(plan, full_map, gate)
    slab, half_slab = make_keys(plan, full_map, rank)
    counts = counts.reshape(-1)[:hidden]

    def wire(rows, d):
        return lax.ppermute(rows, "tp", [(i, (i + d * pair) % tp) for i in range(tp)])

    width = gate_weight.shape[0]

    def across(rows, groups_of_boxes, ready=()):
        sides = []
        for d in range(1, groups):
            packed = list(ready[d - 1 : d])
            for boxes in groups_of_boxes:
                packed += pack_rows(plan, send[d - 1], rows, boxes)
            here = [wire(part, d) for part in packed]
            there = [swap(part) for part in here]
            sides += [here] + [list(side) for side in zip(*there)]
        return sides

    def flat(sides):
        return [part for side in sides for part in side]

    def collect(slab, local, sides, spare, **more):
        tables = local + flat(sides)
        at, resident = len(local), []
        for i, side in enumerate(sides):
            resident += range(at, at + len(side)) if i % pair else []
            at += len(side)
        return collect_rows(plan, top, slab, tables, resident, spare, **more)

    halves = plan.halves
    column = width // halves
    gate_local = [gate] + swap(gate)
    up_local = [up] + swap(up)
    gate_far = across(gate, [[(plan.head, slots, 0, width)]], heads)
    up_far = across(up, [[(0, slots, 0, width)]])
    kept_down = (down_weight.astype(F32) / counts[:, None]).astype(BF16)
    down_boxes = [(0, slots, h * column, (h + 1) * column) for h in range(halves)]
    down_far = across(kept_down, [down_boxes])
    down_local = [kept_down] + swap(kept_down)
    spare = [[], [], []]
    if groups > 1 and plan.rest > 0:
        sides = tp - pair
        rooms = tuple(unwritten((plan.rest, width)) for _ in range(3 * sides))

        def again(state):
            filled = []
            for rows in (gate, up, kept_down):
                filled += flat(across(rows, [[(slots, hidden, 0, width)]]))
            return (jnp.bool_(False), *filled)

        _, *rooms = lax.while_loop(lambda state: state[0], again, (top[0] > slots, *rooms))
        spare = [rooms[i * sides : (i + 1) * sides] for i in range(3)]
    added_gate = collect(slab, gate_local, gate_far, spare[0])
    added_up = collect(slab, up_local, up_far, spare[1])
    added_down = None
    for h in range(halves):
        sides = [[side[h]] for side in down_far]
        added_down = collect(
            half_slab, down_local, sides, spare[2], half=h, halves=halves, running=added_down
        )
    return (added_gate.T, added_up.T, kept_down, added_down)


def solution(mesh):
    return jax.shard_map(
        on_device,
        mesh=mesh,
        in_specs=(P("fsdp", "tp"), P("fsdp", "tp"), P("tp", "fsdp"), P(("fsdp", "tp"))),
        out_specs=(P("fsdp", "tp"), P("fsdp", "tp"), P("tp", "fsdp"), P("tp", "fsdp")),
        check_vma=False,
    )
```
